16 devices in a mesh: task: 4 (over z, y), row: 4 (over x, core).
Axes of the slice: x: 2, y: 2, z: 2, core: 2. Of those that a mesh axis runs over, the one named last changes fastest.
Arguments:
- points: bfloat16 [65536, 768], P(('task', 'row')), parts along dimension 0
- vectors: bfloat16 [65536, 128], P(('task', 'row')), parts along dimension 0
- length_scale: float32 [4], P('task'), parts along dimension 0
- out_scale: float32 [4], P('task'), parts along dimension 0
Outputs:
- output: float32 [65536, 128], P(('task', 'row')), parts along dimension 0
There are 4 independent parts. The reference program is written for one: setup_inputs(seed, part) draws one part's arguments, and reference() takes and returns one part's arrays. A program takes and returns all parts, laid end to end along the dimension named above; each array names one.
All inputs are finite; a program needn't handle non-finite values.
Results may differ from the reference program's by a relative error of at most 0.001.
Values are sent between devices in bfloat16 or wider.
A program may use at most 1 GiB of HBM per device.

```python
import jax
import jax.numpy as jnp
from jax import lax

ROWS_DEV = 4096
GROUP = 4
FEAT = 768
COLS = 128
N_POINTS = GROUP * ROWS_DEV


def setup_inputs(seed: int = 0, part: int = 0) -> dict:
    base_key = jax.random.fold_in(jax.random.key(seed), part)
    key_x, key_o, key_m, key_v, key_l, key_s = jax.random.split(base_key, 6)
    base_pts = jax.random.normal(key_x, (GROUP, ROWS_DEV, FEAT), jnp.float32)
    offset = 1.6 * jax.random.normal(key_o, (GROUP, 1, FEAT), jnp.float32)
    points = (base_pts + offset).reshape(N_POINTS, FEAT).astype(jnp.bfloat16)
    block_mean = jax.random.normal(key_m, (GROUP, 1, COLS), jnp.float32)
    block_mean = block_mean - jnp.mean(block_mean, axis=0, keepdims=True)
    noise_val = 0.5 * jax.random.normal(key_v, (GROUP, ROWS_DEV, COLS), jnp.float32)
    vectors = (block_mean + noise_val).reshape(N_POINTS, COLS).astype(jnp.bfloat16)
    ell_ratio = jax.random.uniform(key_l, (1,), jnp.float32, 0.8, 1.25)
    length_scale = jnp.sqrt(2.0 * FEAT * ell_ratio)
    out_scale = jax.random.uniform(key_s, (1,), jnp.float32, 1.0, 2.0) / ROWS_DEV
    return {"points": points, "vectors": vectors, "length_scale": length_scale, "out_scale": out_scale}


def kernel_tile(x_rows, x_cols, length_scale, out_scale):
    norm_rows = jnp.sum(jnp.square(x_rows.astype(jnp.float32)), axis=1)
    norm_cols = jnp.sum(jnp.square(x_cols.astype(jnp.float32)), axis=1)
    gram_mat = jnp.dot(x_rows, x_cols.T, preferred_element_type=jnp.float32)
    sq_dist = jnp.maximum(norm_rows[:, None] + norm_cols[None, :] - 2.0 * gram_mat, 0.0)
    return (out_scale * jnp.exp(-sq_dist / (2.0 * length_scale * length_scale))).astype(jnp.bfloat16)


def kernel_apply(points, vectors, length_scale, out_scale):
    x_blocks = points.reshape(GROUP, ROWS_DEV, FEAT)
    v_blocks = vectors.reshape(GROUP, ROWS_DEV, COLS)

    def row_block(x_rows):
        def col_step(running, col_pair):
            x_cols, v_cols = col_pair
            kern_tile = kernel_tile(x_rows, x_cols, length_scale, out_scale)
            return running + jnp.dot(kern_tile, v_cols, preferred_element_type=jnp.float32), None

        running, _ = lax.scan(col_step, jnp.zeros((ROWS_DEV, COLS), jnp.float32), (x_blocks, v_blocks))
        return running

    return lax.map(row_block, x_blocks).reshape(N_POINTS, COLS)


def reference(points, vectors, length_scale, out_scale):
    first_pass = kernel_apply(points, vectors, length_scale, out_scale).astype(jnp.bfloat16)
    return kernel_apply(points, first_pass, length_scale, out_scale)
```

```python
import functools

import jax
import jax.numpy as jnp
from jax import lax
from jax.experimental import pallas as pl
from jax.experimental.pallas import tpu as pltpu
from jax.sharding import PartitionSpec as P

MESH = pl.DeviceIdType.MESH
F32 = jnp.float32
BF16 = jnp.bfloat16
LOG2E = 1.4426950408889634

ROWS = 4096
FEAT = 768
COLS = 128
CH = 512
NB = ROWS // CH
NQ = 4 * NB
TI = 256
NT = ROWS // TI
NS = 7
NSTREAM = 3
NKEEP = NS - NSTREAM
NH = NQ - NKEEP


def body(x_ref, v_ref, ell_ref, s_ref, w_ref, k_hbm, xp_hbm,
         xbuf, xt, vg, yg, vt, hj, hi, acc, slots,
         px_s, px_r, pv_s, pv_r, x_s, x_r, v_s, v_r, fx_s, fx_r, fv_s, fv_r,
         yp_s, yp_r, yx_s, yx_r, yf_s, yf_r, st_sem, vl_sem, ko_sem, kl_sem):
    task = lax.axis_index("task")
    me = lax.axis_index("row")
    partner = me + 1 - 2 * lax.rem(me, 2)
    peer = lax.rem(me + 2, 4)

    barrier = pltpu.get_barrier_semaphore()
    for dev in (partner, peer):
        pl.semaphore_signal(barrier, inc=1, device_id=(task, dev), device_id_type=MESH)
    pl.semaphore_wait(barrier, 2)

    def remote(src, dst, send, recv, dev):
        return pltpu.make_async_remote_copy(
            src_ref=src, dst_ref=dst, send_sem=send, recv_sem=recv,
            device_id=(task, dev), device_id_type=MESH)

    def x_cross(k):
        return remote(x_ref.at[k], xbuf.at[2 + 2 * k], x_s.at[k], x_r.at[k], peer)

    def v_cross(k):
        return remote(v_ref.at[k], vg.at[16 + 2 * k], v_s.at[k], v_r.at[k], peer)

    def x_fwd(k):
        return remote(xbuf.at[2 + 2 * k], xbuf.at[3 + 2 * k], fx_s.at[k], fx_r.at[k], partner)

    def v_fwd(k):
        return remote(vg.at[16 + 2 * k], vg.at[17 + 2 * k], fv_s.at[k], fv_r.at[k], partner)

    x_part = remote(x_ref, xp_hbm, px_s, px_r, partner)
    v_part = remote(v_ref, vg.at[pl.ds(NB, NB)], pv_s, pv_r, partner)

    def y_part(k):
        return remote(yg.at[k], yg.at[NB + k], yp_s.at[k], yp_r.at[k], partner)

    def y_cross(k):
        return remote(yg.at[k], yg.at[16 + 2 * k], yx_s.at[k], yx_r.at[k], peer)

    def y_fwd(k):
        return remote(yg.at[16 + 2 * k], yg.at[17 + 2 * k], yf_s.at[k], yf_r.at[k], partner)

    def stage_own(k, buf):
        return pltpu.make_async_copy(x_ref.at[k], xbuf.at[buf], st_sem.at[buf])

    def stage_part(k, buf):
        return pltpu.make_async_copy(xp_hbm.at[k], xbuf.at[buf], st_sem.at[buf])

    def k_out(q, slot):
        return pltpu.make_async_copy(slots.at[slot], k_hbm.at[q], ko_sem.at[slot])

    def k_load(q, slot):
        return pltpu.make_async_copy(k_hbm.at[q], slots.at[slot], kl_sem.at[slot])

    v_own = pltpu.make_async_copy(v_ref, vg.at[pl.ds(0, NB)], vl_sem)

    stage_own(0, 0).start()

    @pl.loop(0, NB)
    def _(k):
        v_cross(k).start()
        x_cross(k).start()

    v_part.start()
    x_part.start()
    v_own.start()

    @pl.loop(0, NB)
    def _(k):
        buf = lax.rem(k, 2)

        @pl.when(k + 1 < NB)
        def _():
            stage_own(k + 1, 1 - buf).start()

        stage_own(k, buf).wait()
        xc = xbuf[buf]
        cols = pl.ds(pl.multiple_of(k * CH, CH), CH)
        xct = xc.T
        xt[:, cols] = xct
        hi[:, cols] = 0.5 * jnp.sum(jnp.square(xct.astype(F32)), axis=0, keepdims=True)

    stage_own(0, 0).start()
    acc[...] = jnp.zeros_like(acc)
    v_own.wait()

    ell = ell_ref[0]
    s = s_ref[0]
    ratio = jnp.full((8, 128), -2.0 * LOG2E, F32) / jnp.full((8, 128), 2.0 * ell * ell, F32)
    scale_e = ratio[0:1, :]

    @pl.loop(0, NQ)
    def _(q):
        k = lax.div(q - 16, 2)
        slot = lax.rem(q, NS)

        @pl.when(jnp.logical_and(q >= 1, q - 1 < NH))
        def _():
            k_out(q - 1, lax.rem(q - 1 + NS, NS)).start()

        @pl.when(q >= NS)
        def _():
            k_out(q - NS, slot).wait()

        @pl.when(q == 7)
        def _():
            x_part.wait_recv()
            v_part.wait_recv()

        @pl.when(q < 7)
        def _():
            stage_own(q + 1, lax.rem(q + 1, 2)).start()

        @pl.when(jnp.logical_and(q >= 7, q < 15))
        def _():
            stage_part(q - 7, lax.rem(q + 1, 2)).start()

        @pl.when(q < 16)
        def _():
            stage_own(0, lax.rem(q, 2)).wait()

        @pl.when(jnp.logical_and(q >= 16, lax.rem(q, 2) == 0))
        def _():
            x_cross(k).wait_recv()
            x_fwd(k).start()
            v_cross(k).wait_recv()
            v_fwd(k).start()

        @pl.when(jnp.logical_and(q >= 16, lax.rem(q, 2) == 1))
        def _():
            x_fwd(k).wait_recv()
            v_fwd(k).wait_recv()

        xi = jnp.where(q < 16, lax.rem(q, 2), q - 14)
        xc_ref = xbuf.at[xi]
        vt[...] = vg[q].T
        hj[...] = jnp.broadcast_to(
            0.5 * jnp.sum(jnp.square(xc_ref[...].astype(F32)), axis=1, keepdims=True), (CH, 128))

        def gen(t):
            cols = pl.ds(t * TI, TI)
            g = jnp.dot(xc_ref[...], xt[:, cols], preferred_element_type=F32)
            h = jnp.concatenate([hj[...]] * (TI // 128), axis=1)
            c = jnp.concatenate([scale_e] * (TI // 128), axis=1)
            d = jnp.maximum(h + hi[:, cols] - g, 0.0)
            slots[slot, :, cols] = (s * jnp.exp2(d * c)).astype(BF16)

        def app(t):
            cols = pl.ds(t * TI, TI)
            acc[:, cols] += jnp.dot(vt[...], slots[slot, :, cols], preferred_element_type=F32)

        for t in range(NT + 2):
            if t < NT:
                gen(t)
            if t >= 2:
                app(t - 2)

    for k in range(NB + 1):
        if k < NB:
            yg[k] = acc[:, k * CH:(k + 1) * CH].astype(BF16)
        if k >= 1:
            y_cross(k - 1).start()
            y_part(k - 1).start()
    acc[...] = jnp.zeros_like(acc)

    @pl.loop(0, NSTREAM)
    def _(i):
        k_out(NH - NSTREAM + i, NKEEP + i).wait()
        k_load(i, NKEEP + i).start()

    @pl.loop(0, NQ)
    def _(q):
        k = lax.div(q - 16, 2)
        slot = jnp.where(q < NH, NKEEP + lax.rem(q, NSTREAM), q - NH)

        @pl.when(jnp.logical_and(q >= NB, q < 16))
        def _():
            y_part(q - NB).wait_recv()

        @pl.when(q == 16)
        def _():
            y_cross(0).wait_recv()
            y_fwd(0).start()

        @pl.when(jnp.logical_and(jnp.logical_and(q >= 16, lax.rem(q, 2) == 0), k + 1 < NB))
        def _():
            y_cross(k + 1).wait_recv()
            y_fwd(k + 1).start()

        @pl.when(jnp.logical_and(q >= 16, lax.rem(q, 2) == 1))
        def _():
            y_fwd(k).wait_recv()

        @pl.when(q < NH)
        def _():
            k_load(q, slot).wait()

        for t in range(ROWS // 512):
            cols = pl.ds(t * 512, 512)
            acc[:, cols] += jnp.dot(yg[q], slots[slot, :, cols], preferred_element_type=F32)

        @pl.when(q + NSTREAM < NH)
        def _():
            k_load(q + NSTREAM, slot).start()

    for t in range(ROWS // 512):
        w_ref[t * 512:(t + 1) * 512, :] = acc[:, t * 512:(t + 1) * 512].T

    x_part.wait_send()
    v_part.wait_send()

    @pl.loop(0, NB)
    def _(k):
        x_cross(k).wait_send()
        v_cross(k).wait_send()
        x_fwd(k).wait_send()
        v_fwd(k).wait_send()
        y_part(k).wait_send()
        y_cross(k).wait_send()
        y_fwd(k).wait_send()


def solution(mesh):
    def local_program(x_loc, v_loc, length_scale, out_scale):
        dma = pltpu.SemaphoreType.DMA
        any_spec = pl.BlockSpec(memory_space=pl.ANY)
        smem = pl.BlockSpec(memory_space=pltpu.SMEM)
        out = pl.pallas_call(
            body,
            out_shape=[
                jax.ShapeDtypeStruct((ROWS, COLS), F32),
                jax.ShapeDtypeStruct((NH, CH, ROWS), BF16),
                jax.ShapeDtypeStruct((NB, CH, FEAT), BF16),
            ],
            in_specs=[any_spec, any_spec, smem, smem],
            out_specs=[pl.BlockSpec(memory_space=pltpu.VMEM), any_spec, any_spec],
            scratch_shapes=[
                pltpu.VMEM((2 + 2 * NB, CH, FEAT), BF16),
                pltpu.VMEM((FEAT, ROWS), BF16),
                pltpu.VMEM((NQ, CH, COLS), BF16),
                pltpu.VMEM((NQ, COLS, CH), BF16),
                pltpu.VMEM((COLS, CH), BF16),
                pltpu.VMEM((CH, 128), F32),
                pltpu.VMEM((1, ROWS), F32),
                pltpu.VMEM((COLS, ROWS), F32),
                pltpu.VMEM((NS, CH, ROWS), BF16),
                dma, dma, dma, dma,
                dma((NB,)), dma((NB,)), dma((NB,)), dma((NB,)),
                dma((NB,)), dma((NB,)), dma((NB,)), dma((NB,)),
                dma((NB,)), dma((NB,)), dma((NB,)), dma((NB,)), dma((NB,)), dma((NB,)),
                dma((2,)), dma, dma((NS,)), dma((NS,)),
            ],
            compiler_params=pltpu.CompilerParams(
                collective_id=0, has_side_effects=True, vmem_limit_bytes=67043328),
            name="two_products",
        )(x_loc.reshape(NB, CH, FEAT), v_loc.reshape(NB, CH, COLS), length_scale, out_scale)
        return out[0]

    row_spec = P(("task", "row"), None)
    return jax.shard_map(local_program, mesh=mesh, in_specs=(row_spec, row_spec, P("task"), P("task")),
                         out_specs=row_spec, check_vma=False)
```

```python
import jax
import jax.numpy as jnp
from jax import lax
from jax.experimental import pallas as pl
from jax.experimental.pallas import tpu as pltpu
from jax.sharding import PartitionSpec as P

MESH = pl.DeviceIdType.MESH
F32 = jnp.float32
BF16 = jnp.bfloat16
LOG2E = 1.4426950408889634

ROWS = 4096
FEAT = 768
COLS = 128
CH = 512
NB = ROWS // CH
NQ = 4 * NB
NM = NQ - 1
NL = NQ - 2
TI = 256
NT = ROWS // TI
HALF = CH // 2
NS = 11
NSTREAM = 3
NH = NQ - (NS - NSTREAM)


def body(x_ref, v_ref, ell_ref, s_ref, w_ref, k_hbm, xg, vg,
         xbuf, vbuf, xt, yg, vt, hj, hi, acc, wacc, slots,
         px_s, px_r, pv_s, pv_r, x_s, x_r, v_s, v_r, fx_s, fx_r, fv_s, fv_r,
         yp_s, yp_r, yx_s, yx_r, yf_s, yf_r, st_sem, sv_sem, ko_sem, kl_sem):
    task = lax.axis_index("task")
    me = lax.axis_index("row")
    partner = me + 1 - 2 * lax.rem(me, 2)
    peer = lax.rem(me + 2, 4)

    barrier = pltpu.get_barrier_semaphore()
    for dev in (peer, partner):
        pl.semaphore_signal(barrier, inc=1, device_id=(task, dev), device_id_type=MESH)
    pl.semaphore_wait(barrier, 2)

    def remote(src, dst, send, recv, dev):
        return pltpu.make_async_remote_copy(
            src_ref=src, dst_ref=dst, send_sem=send, recv_sem=recv,
            device_id=(task, dev), device_id_type=MESH)

    def x_cross(k):
        return remote(x_ref.at[k], xg.at[8 + 2 * k], x_s.at[k], x_r.at[k], peer)

    def v_cross(k):
        return remote(v_ref.at[k], vg.at[8 + 2 * k], v_s.at[k], v_r.at[k], peer)

    def x_fwd(k):
        return remote(xg.at[8 + 2 * k], xg.at[9 + 2 * k], fx_s.at[k], fx_r.at[k], partner)

    def v_fwd(k):
        return remote(vg.at[8 + 2 * k], vg.at[9 + 2 * k], fv_s.at[k], fv_r.at[k], partner)

    last = NB - 1
    def halves(r, i):
        return r.at[pl.ds(i * HALF, HALF)]

    x_last = [remote(halves(x_ref.at[last], i), halves(xbuf.at[2 + i], 0), x_s.at[last + i], x_r.at[last + i], peer)
              for i in range(2)]
    v_last = [remote(halves(v_ref.at[last], i), halves(vbuf.at[2 + i], 0), v_s.at[last + i], v_r.at[last + i], peer)
              for i in range(2)]
    x_last_fwd = [remote(halves(xbuf.at[2 + i], 0), halves(xbuf.at[2 + i], 1),
                         fx_s.at[last + i], fx_r.at[last + i], partner) for i in range(2)]
    v_last_fwd = [remote(halves(vbuf.at[2 + i], 0), halves(vbuf.at[2 + i], 1),
                         fv_s.at[last + i], fv_r.at[last + i], partner) for i in range(2)]

    def receive_last(i):
        v_last[i].wait_recv()
        v_last_fwd[i].start()
        x_last[i].wait_recv()
        x_last_fwd[i].start()
        v_last_fwd[i].wait_recv()
        x_last_fwd[i].wait_recv()

    x_part = remote(x_ref, xg.at[pl.ds(0, NB)], px_s, px_r, partner)
    v_part = remote(v_ref, vg.at[pl.ds(0, NB)], pv_s, pv_r, partner)

    def y_part(k):
        return remote(yg.at[k], yg.at[NB + k], yp_s.at[k], yp_r.at[k], partner)

    def y_cross(k):
        return remote(yg.at[k], yg.at[16 + 2 * k], yx_s.at[k], yx_r.at[k], peer)

    def y_fwd(k):
        return remote(yg.at[16 + 2 * k], yg.at[17 + 2 * k], yf_s.at[k], yf_r.at[k], partner)

    def y_piece(k, i):
        return yg.at[k, :, pl.ds(i * HALF, HALF)]

    y_last = [remote(y_piece(last, i), y_piece(NL + i, 0), yx_s.at[last + i], yx_r.at[last + i], peer)
              for i in range(2)]
    y_last_fwd = [remote(y_piece(NL + i, 0), y_piece(NL + i, 1), yf_s.at[last + i], yf_r.at[last + i], partner)
                  for i in range(2)]

    class Stage:
        def __init__(self, x_src, v_src, buf):
            self.x = pltpu.make_async_copy(x_src, xbuf.at[buf], st_sem.at[buf])
            self.v = pltpu.make_async_copy(v_src, vbuf.at[buf], sv_sem.at[buf])

        def start(self):
            self.x.start()
            self.v.start()

        def wait(self):
            self.x.wait()
            self.v.wait()

    def stage_own(q):
        return Stage(x_ref.at[q], v_ref.at[q], lax.rem(q, 2))

    def stage_got(q):
        return Stage(xg.at[q - NB], vg.at[q - NB], lax.rem(q, 2))

    def k_out(q):
        slot = lax.rem(q, NS)
        return pltpu.make_async_copy(slots.at[slot], k_hbm.at[q], ko_sem.at[slot])

    def stream_slot(q):
        return lax.rem(NH - NSTREAM + lax.rem(q, NSTREAM), NS)

    def k_load(q):
        slot = stream_slot(q)
        return pltpu.make_async_copy(k_hbm.at[q], slots.at[slot], kl_sem.at[slot])

    stage_own(0).start()

    @pl.loop(0, last)
    def _(k):
        v_cross(k).start()
        x_cross(k).start()

    for v, x in zip(v_last, x_last):
        v.start()
        x.start()
    v_part.start()
    x_part.start()

    @pl.loop(0, NB)
    def _(k):
        @pl.when(k + 1 < NB)
        def _():
            stage_own(k + 1).start()

        stage_own(k).wait()
        xct = xbuf[lax.rem(k, 2)].T
        cols = pl.ds(pl.multiple_of(k * CH, CH), CH)
        xt[:, cols] = xct
        hi[:, cols] = 0.5 * jnp.sum(jnp.square(xct.astype(F32)), axis=0, keepdims=True)

    stage_own(0).start()
    acc[...] = jnp.zeros_like(acc)
    wacc[...] = jnp.zeros_like(wacc)

    ell = ell_ref[0]
    s = s_ref[0]
    ratio = jnp.full((8, 128), -2.0 * LOG2E, F32) / jnp.full((8, 128), 2.0 * ell * ell, F32)
    scale_e = ratio[0:1, :]

    def prepare(x_i, h_i):
        vt[h_i] = vbuf[x_i].T
        hj[h_i] = jnp.broadcast_to(
            0.5 * jnp.sum(jnp.square(xbuf[x_i].astype(F32)), axis=1, keepdims=True), (CH, 128))

    def gen(x_i, h_i, slot, cols, width):
        g = jnp.dot(xbuf[x_i], xt[:, cols], preferred_element_type=F32)
        h = jnp.concatenate([hj[h_i]] * (width // 128), axis=1)
        c = jnp.concatenate([scale_e] * (width // 128), axis=1)
        d = jnp.maximum(h + hi[:, cols] - g, 0.0)
        slots[slot, :, cols] = (s * jnp.exp2(d * c)).astype(BF16)

    @pl.loop(0, NM)
    def _(q):
        slot = lax.rem(q, NS)
        n = q + 1
        k = lax.div(n - 16, 2)

        @pl.when(jnp.logical_and(q >= 1, q - 1 < NH))
        def _():
            k_out(q - 1).start()

        @pl.when(q >= NS)
        def _():
            k_out(q - NS).wait()

        @pl.when(q >= NM - NSTREAM)
        def _():
            i = q - (NM - NSTREAM)
            k_out(NH - NSTREAM + i).wait()
            k_load(i).start()

        @pl.when(n < NB)
        def _():
            stage_own(n).start()

        @pl.when(n == NB)
        def _():
            x_part.wait_recv()
            v_part.wait_recv()

        @pl.when(jnp.logical_and(n >= 16, n < NL))
        def _():
            @pl.when(lax.rem(n, 2) == 0)
            def _():
                v_cross(k).wait_recv()
                v_fwd(k).start()
                x_cross(k).wait_recv()
                x_fwd(k).start()

            @pl.when(lax.rem(n, 2) == 1)
            def _():
                v_fwd(k).wait_recv()
                x_fwd(k).wait_recv()

        @pl.when(jnp.logical_and(n >= NB, n < NL))
        def _():
            stage_got(n).start()

        @pl.when(q < NL)
        def _():
            stage_own(lax.rem(q, 2)).wait()

        @pl.when(q == NL)
        def _():
            receive_last(0)

        x_i = jnp.where(q < NL, lax.rem(q, 2), 2)
        prepare(x_i, 0)

        def app(t):
            cols = pl.ds(t * TI, TI)
            acc[:, cols] += jnp.dot(vt[0], slots[slot, :, cols], preferred_element_type=F32)

        for t in range(NT + 2):
            if t < NT:
                gen(x_i, 0, slot, pl.ds(t * TI, TI), TI)
            if t >= 2:
                app(t - 2)

    receive_last(1)
    prepare(3, 0)
    slot_b = (NQ - 1) % NS
    k_out(NQ - 1 - NS).wait()

    def second(q, slot):
        for t in range(ROWS // 512):
            cols = pl.ds(t * 512, 512)
            wacc[:, cols] += jnp.dot(yg[q], slots[slot, :, cols], preferred_element_type=F32)

    def second_streamed(q):
        k_load(q).wait()
        second(q, stream_slot(q))

        @pl.when(q + NSTREAM < NH)
        def _():
            k_load(q + NSTREAM).start()

    @pl.loop(0, NB + 1)
    def _(t):
        @pl.when(t < NB)
        def _():
            cols = pl.ds(pl.multiple_of(t * CH, CH), CH)
            gen(3, 0, slot_b, cols, CH)
            y = acc[:, cols] + jnp.dot(vt[0], slots[slot_b, :, cols], preferred_element_type=F32)
            yg[t] = y.astype(BF16)

        @pl.when(t >= 1)
        def _():
            @pl.when(t < NB)
            def _():
                y_cross(t - 1).start()

            @pl.when(t == NB)
            def _():
                y_last[0].start()
                y_last[1].start()

            y_part(t - 1).start()
            second_streamed(t - 1)

    @pl.loop(0, NB)
    def _(i):
        @pl.when(i < last)
        def _():
            y_cross(i).wait_recv()
            y_fwd(i).start()

        @pl.when(i == last)
        def _():
            for c, f in zip(y_last, y_last_fwd):
                c.wait_recv()
                f.start()

        y_part(i).wait_recv()
        second_streamed(NB + i)

    @pl.loop(0, NB)
    def _(i):
        q, r = 16 + i, NH + i
        k = lax.div(i, 2)

        @pl.when(lax.rem(i, 2) == 1)
        def _():
            y_fwd(k).wait_recv()

            @pl.when(k + 4 < last)
            def _():
                y_fwd(k + 4).wait_recv()

        @pl.when(i == 6)
        def _():
            for f in y_last_fwd:
                f.wait_recv()

        k_load(q).wait()
        sq, sr = stream_slot(q), lax.rem(r, NS)
        for t in range(ROWS // 512):
            cols = pl.ds(t * 512, 512)
            wacc[:, cols] += (jnp.dot(yg[q], slots[sq, :, cols], preferred_element_type=F32)
                              + jnp.dot(yg[r], slots[sr, :, cols], preferred_element_type=F32))

        @pl.when(q + NSTREAM < NH)
        def _():
            k_load(q + NSTREAM).start()

    out = pltpu.make_async_copy(wacc, w_ref, px_s)
    x_part.wait_send()
    out.start()
    v_part.wait_send()

    @pl.loop(0, last)
    def _(k):
        x_cross(k).wait_send()
        v_cross(k).wait_send()
        x_fwd(k).wait_send()
        v_fwd(k).wait_send()

    for c in (*x_last, *x_last_fwd, *v_last, *v_last_fwd, *y_last, *y_last_fwd):
        c.wait_send()

    @pl.loop(0, last)
    def _(k):
        y_part(k).wait_send()
        y_cross(k).wait_send()
        y_fwd(k).wait_send()

    y_part(last).wait_send()

    out.wait()


def solution(mesh):
    def local_program(x_loc, v_loc, length_scale, out_scale):
        dma = pltpu.SemaphoreType.DMA
        any_spec = pl.BlockSpec(memory_space=pl.ANY)
        smem = pl.BlockSpec(memory_space=pltpu.SMEM)
        out = pl.pallas_call(
            body,
            out_shape=[
                jax.ShapeDtypeStruct((COLS, ROWS), F32),
                jax.ShapeDtypeStruct((NH, CH, ROWS), BF16),
                jax.ShapeDtypeStruct((NL - NB, CH, FEAT), BF16),
                jax.ShapeDtypeStruct((NL - NB, CH, COLS), BF16),
            ],
            in_specs=[any_spec, any_spec, smem, smem],
            out_specs=[any_spec] * 4,
            scratch_shapes=[
                pltpu.VMEM((4, CH, FEAT), BF16),
                pltpu.VMEM((4, CH, COLS), BF16),
                pltpu.VMEM((FEAT, ROWS), BF16),
                pltpu.VMEM((NQ, COLS, CH), BF16),
                pltpu.VMEM((1, COLS, CH), BF16),
                pltpu.VMEM((1, CH, 128), F32),
                pltpu.VMEM((1, ROWS), F32),
                pltpu.VMEM((COLS, ROWS), F32),
                pltpu.VMEM((COLS, ROWS), F32),
                pltpu.VMEM((NS, CH, ROWS), BF16),
                dma, dma, dma, dma,
                *[dma((NB + 1,))] * 14,
                dma((2,)), dma((2,)), dma((NS,)), dma((NS,)),
            ],
            compiler_params=pltpu.CompilerParams(
                collective_id=0, has_side_effects=True, vmem_limit_bytes=67043328),
            name="two_products",
        )(x_loc.reshape(NB, CH, FEAT), v_loc.reshape(NB, CH, COLS), length_scale, out_scale)
        return out[0].T

    row_spec = P(("task", "row"), None)
    return jax.shard_map(local_program, mesh=mesh, in_specs=(row_spec, row_spec, P("task"), P("task")),
                         out_specs=row_spec, check_vma=False)
```

```python
import jax
import jax.numpy as jnp
from jax import lax
from jax.experimental import pallas as pl
from jax.experimental.pallas import tpu as pltpu
from jax.sharding import PartitionSpec as P

MESH = pl.DeviceIdType.MESH
F32 = jnp.float32
BF16 = jnp.bfloat16
LOG2E = 1.4426950408889634

ROWS = 4096
FEAT = 768
COLS = 128
CH = 512
NB = ROWS // CH
NQ = 4 * NB
NM = NQ - 1
NL = NQ - 2
TI = 256
NT = ROWS // TI
HALF = CH // 2
LATE = 26
PIECES = ((0, 256, 0, 0), (256, 128, 1, 0), (384, 128, 1, 256))
NS = 11
NSTREAM = 3
NH = NQ - (NS - NSTREAM)


def body(x_ref, v_ref, ell_ref, s_ref, w_ref, k_hbm, xg, vg,
         xbuf, vbuf, xt, yg, vt, hj, hi, acc, wacc, slots,
         px_s, px_r, pv_s, pv_r, x_s, x_r, v_s, v_r, fx_s, fx_r, fv_s, fv_r,
         yp_s, yp_r, yx_s, yx_r, yf_s, yf_r, st_sem, sv_sem, ko_sem, kl_sem):
    task = lax.axis_index("task")
    me = lax.axis_index("row")
    partner = me + 1 - 2 * lax.rem(me, 2)
    peer = lax.rem(me + 2, 4)

    barrier = pltpu.get_barrier_semaphore()
    for dev in (peer, partner):
        pl.semaphore_signal(barrier, inc=1, device_id=(task, dev), device_id_type=MESH)
    pl.semaphore_wait(barrier, 2)

    def remote(src, dst, send, recv, dev):
        return pltpu.make_async_remote_copy(
            src_ref=src, dst_ref=dst, send_sem=send, recv_sem=recv,
            device_id=(task, dev), device_id_type=MESH)

    def x_cross(k):
        return remote(x_ref.at[k], xg.at[8 + 2 * k], x_s.at[k], x_r.at[k], peer)

    def v_cross(k):
        return remote(v_ref.at[k], vg.at[8 + 2 * k], v_s.at[k], v_r.at[k], peer)

    def x_fwd(k):
        return remote(xg.at[8 + 2 * k], xg.at[9 + 2 * k], fx_s.at[k], fx_r.at[k], partner)

    def v_fwd(k):
        return remote(vg.at[8 + 2 * k], vg.at[9 + 2 * k], fv_s.at[k], fv_r.at[k], partner)

    last = NB - 1
    x_last, v_last, y_last, x_last_fwd, v_last_fwd, y_last_fwd = [], [], [], [], [], []
    for i, (row, size, c, to) in enumerate(PIECES):
        src, dst, fwd = pl.ds(row, size), pl.ds(to, size), pl.ds(to + size, size)
        n = last + i
        x_last.append(remote(x_ref.at[last, src], xbuf.at[2 + c, dst], x_s.at[n], x_r.at[n], peer))
        v_last.append(remote(v_ref.at[last, src], vbuf.at[2 + c, dst], v_s.at[n], v_r.at[n], peer))
        y_last.append(remote(yg.at[last, :, src], yg.at[NL + c, :, dst], yx_s.at[n], yx_r.at[n], peer))
        x_last_fwd.append(remote(xbuf.at[2 + c, dst], xbuf.at[2 + c, fwd], fx_s.at[n], fx_r.at[n], partner))
        v_last_fwd.append(remote(vbuf.at[2 + c, dst], vbuf.at[2 + c, fwd], fv_s.at[n], fv_r.at[n], partner))
        y_last_fwd.append(remote(yg.at[NL + c, :, dst], yg.at[NL + c, :, fwd], yf_s.at[n], yf_r.at[n], partner))

    def receive_last(i):
        x_last[i].wait_recv()
        x_last_fwd[i].start()
        v_last[i].wait_recv()
        v_last_fwd[i].start()
        x_last_fwd[i].wait_recv()
        v_last_fwd[i].wait_recv()

    x_part = remote(x_ref, xg.at[pl.ds(0, NB)], px_s, px_r, partner)
    v_part = remote(v_ref, vg.at[pl.ds(0, NB)], pv_s, pv_r, partner)

    def y_part(k):
        return remote(yg.at[k], yg.at[NB + k], yp_s.at[k], yp_r.at[k], partner)

    def y_cross(k):
        return remote(yg.at[k], yg.at[16 + 2 * k], yx_s.at[k], yx_r.at[k], peer)

    def y_fwd(k):
        return remote(yg.at[16 + 2 * k], yg.at[17 + 2 * k], yf_s.at[k], yf_r.at[k], partner)

    class Stage:
        def __init__(self, x_src, v_src, buf):
            self.x = pltpu.make_async_copy(x_src, xbuf.at[buf], st_sem.at[buf])
            self.v = pltpu.make_async_copy(v_src, vbuf.at[buf], sv_sem.at[buf])

        def start(self):
            self.x.start()
            self.v.start()

        def wait(self):
            self.x.wait()
            self.v.wait()

    def stage_own(q):
        return Stage(x_ref.at[q], v_ref.at[q], lax.rem(q, 2))

    def stage_got(q):
        return Stage(xg.at[q - NB], vg.at[q - NB], lax.rem(q, 2))

    def k_out(q):
        slot = lax.rem(q, NS)
        return pltpu.make_async_copy(slots.at[slot], k_hbm.at[q], ko_sem.at[slot])

    def stream_slot(q):
        return lax.rem(NH - NSTREAM + lax.rem(q, NSTREAM), NS)

    def k_load(q):
        slot = stream_slot(q)
        return pltpu.make_async_copy(k_hbm.at[q], slots.at[slot], kl_sem.at[slot])

    stage_own(0).start()

    @pl.loop(0, last)
    def _(k):
        v_cross(k).start()
        x_cross(k).start()

    for v, x in zip(v_last, x_last):
        v.start()
        x.start()
    v_part.start()
    x_part.start()

    @pl.loop(0, NB)
    def _(k):
        @pl.when(k + 1 < NB)
        def _():
            stage_own(k + 1).start()

        stage_own(k).wait()
        xct = xbuf[lax.rem(k, 2)].T
        cols = pl.ds(pl.multiple_of(k * CH, CH), CH)
        xt[:, cols] = xct
        hi[:, cols] = 0.5 * jnp.sum(jnp.square(xct.astype(F32)), axis=0, keepdims=True)

    stage_own(0).start()
    acc[...] = jnp.zeros_like(acc)
    wacc[...] = jnp.zeros_like(wacc)

    ell = ell_ref[0]
    s = s_ref[0]
    ratio = jnp.full((8, 128), -2.0 * LOG2E, F32) / jnp.full((8, 128), 2.0 * ell * ell, F32)
    scale_e = ratio[0:1, :]

    def prepare(x_i, rows):
        vt[:, rows] = vbuf[x_i, rows].T
        hj[rows] = jnp.broadcast_to(
            0.5 * jnp.sum(jnp.square(xbuf[x_i, rows].astype(F32)), axis=1, keepdims=True), (rows.size, 128))

    def gen(x_i, rows, slot, cols, width):
        g = jnp.dot(xbuf[x_i, rows], xt[:, cols], preferred_element_type=F32)
        h = jnp.concatenate([hj[rows]] * (width // 128), axis=1)
        c = jnp.concatenate([scale_e] * (width // 128), axis=1)
        d = jnp.maximum(h + hi[:, cols] - g, 0.0)
        slots[slot, rows, cols] = (s * jnp.exp2(d * c)).astype(BF16)

    every = pl.ds(0, CH)

    @pl.loop(0, NM)
    def _(q):
        slot = lax.rem(q, NS)
        n = q + 1
        k = lax.div(n - 16, 2)

        @pl.when(jnp.logical_and(q >= 1, q - 1 < NH))
        def _():
            k_out(q - 1).start()

        @pl.when(q >= NS)
        def _():
            k_out(q - NS).wait()

        @pl.when(q >= NM - NSTREAM)
        def _():
            i = q - (NM - NSTREAM)
            k_out(NH - NSTREAM + i).wait()
            k_load(i).start()

        @pl.when(n < NB)
        def _():
            stage_own(n).start()

        @pl.when(n == NB)
        def _():
            x_part.wait_recv()
            v_part.wait_recv()

        def receive():
            v_cross(k).wait_recv()
            v_fwd(k).start()
            x_cross(k).wait_recv()
            x_fwd(k).start()

        from_peer = jnp.logical_and(n >= 16, lax.rem(n, 2) == 0)
        is_late = jnp.logical_and(jnp.logical_and(from_peer, n >= LATE), n < NL)

        @pl.when(jnp.logical_and(from_peer, n < LATE))
        def _():
            receive()

        @pl.when(jnp.logical_and(jnp.logical_and(n >= 16, lax.rem(n, 2) == 1), n < NL))
        def _():
            v_fwd(k).wait_recv()
            x_fwd(k).wait_recv()

        @pl.when(jnp.logical_and(jnp.logical_and(n >= NB, n < NL), jnp.logical_not(is_late)))
        def _():
            stage_got(n).start()

        @pl.when(q < NL)
        def _():
            stage_own(lax.rem(q, 2)).wait()

        @pl.when(q == NL)
        def _():
            receive_last(0)

        x_i = jnp.where(q < NL, lax.rem(q, 2), 2)
        prepare(x_i, every)

        def app(t):
            cols = pl.ds(t * TI, TI)
            acc[:, cols] += jnp.dot(vt[...], slots[slot, :, cols], preferred_element_type=F32)

        for t in range(NT + 2):
            if t < NT:
                gen(x_i, every, slot, pl.ds(t * TI, TI), TI)
            if t >= 2:
                app(t - 2)

        @pl.when(is_late)
        def _():
            receive()
            stage_got(n).start()

    early, late = pl.ds(0, HALF), pl.ds(HALF, HALF)
    slot_b = (NQ - 1) % NS
    receive_last(1)
    k_out(NQ - 1 - NS).wait()
    prepare(3, early)

    for t in range(NT):
        gen(3, early, slot_b, pl.ds(t * TI, TI), TI)

    receive_last(2)
    prepare(3, late)

    def finish(t):
        cols = pl.ds(pl.multiple_of(t * CH, CH), CH)
        gen(3, late, slot_b, cols, CH)
        y = acc[:, cols] + jnp.dot(vt[...], slots[slot_b, :, cols], preferred_element_type=F32)
        yg[t] = y.astype(BF16)

    def second(q, slot, tiles=range(ROWS // 512)):
        for t in tiles:
            cols = pl.ds(t * 512, 512)
            wacc[:, cols] += jnp.dot(yg[q], slots[slot, :, cols], preferred_element_type=F32)

    def second_streamed(q):
        k_load(q).wait()
        second(q, stream_slot(q))

        @pl.when(q + NSTREAM < NH)
        def _():
            k_load(q + NSTREAM).start()

    finish(0)

    @pl.loop(1, NB)
    def _(t):
        y_cross(t - 1).start()
        y_part(t - 1).start()
        k_load(t - 1).wait()
        finish(t)
        second(t - 1, stream_slot(t - 1))
        k_load(t - 1 + NSTREAM).start()

    for c in y_last:
        c.start()
    y_part(last).start()
    second_streamed(last)

    def forward_y(k):
        y_cross(k).wait_recv()
        y_fwd(k).start()

    @pl.loop(0, NB)
    def _(i):
        @pl.when(i < 3)
        def _():
            forward_y(i)

        @pl.when(jnp.logical_or(i == 4, i == 6))
        def _():
            forward_y(1 + lax.div(i, 2))

        y_part(i).wait_recv()
        second_streamed(NB + i)

    @pl.loop(0, last)
    def _(i):
        q, r = 16 + i, NH + i
        k = lax.div(i, 2)

        @pl.when(jnp.logical_or(i == 2, i == 3))
        def _():
            forward_y(3 + i)

        for j in range(len(PIECES)):
            @pl.when(i == 4 + j)
            def _():
                y_last[j].wait_recv()
                y_last_fwd[j].start()

        @pl.when(lax.rem(i, 2) == 1)
        def _():
            y_fwd(k).wait_recv()
            y_fwd(k + 4).wait_recv()

        @pl.when(i == 6)
        def _():
            y_last_fwd[0].wait_recv()

        k_load(q).wait()
        sq, sr = stream_slot(q), lax.rem(r, NS)
        for t in range(ROWS // 512):
            cols = pl.ds(t * 512, 512)
            wacc[:, cols] += (jnp.dot(yg[q], slots[sq, :, cols], preferred_element_type=F32)
                              + jnp.dot(yg[r], slots[sr, :, cols], preferred_element_type=F32))

        @pl.when(q + NSTREAM < NH)
        def _():
            k_load(q + NSTREAM).start()

    y_fwd(3).wait_recv()
    k_load(NH - 1).wait()
    second(NH - 1, (NH - 1) % NS)
    for f in y_last_fwd[1:]:
        f.wait_recv()

    n_out = 4
    width = ROWS // n_out
    outs = [pltpu.make_async_copy(wacc.at[:, pl.ds(b * width, width)], w_ref.at[:, pl.ds(b * width, width)],
                                  kl_sem.at[b]) for b in range(n_out)]
    for b in range(n_out):
        second(NQ - 1, slot_b, range(b * width // 512, (b + 1) * width // 512))
        if b:
            outs[b - 1].start()
    x_part.wait_send()
    v_part.wait_send()
    outs[-1].start()

    @pl.loop(0, last)
    def _(k):
        x_cross(k).wait_send()
        v_cross(k).wait_send()
        x_fwd(k).wait_send()
        v_fwd(k).wait_send()

    for c in (*x_last, *x_last_fwd, *v_last, *v_last_fwd, *y_last, *y_last_fwd):
        c.wait_send()

    @pl.loop(0, last)
    def _(k):
        y_part(k).wait_send()
        y_cross(k).wait_send()
        y_fwd(k).wait_send()

    y_part(last).wait_send()

    for o in outs:
        o.wait()


def solution(mesh):
    def local_program(x_loc, v_loc, length_scale, out_scale):
        dma = pltpu.SemaphoreType.DMA
        any_spec = pl.BlockSpec(memory_space=pl.ANY)
        smem = pl.BlockSpec(memory_space=pltpu.SMEM)
        out = pl.pallas_call(
            body,
            out_shape=[
                jax.ShapeDtypeStruct((COLS, ROWS), F32),
                jax.ShapeDtypeStruct((NH, CH, ROWS), BF16),
                jax.ShapeDtypeStruct((NL - NB, CH, FEAT), BF16),
                jax.ShapeDtypeStruct((NL - NB, CH, COLS), BF16),
            ],
            in_specs=[any_spec, any_spec, smem, smem],
            out_specs=[any_spec] * 4,
            scratch_shapes=[
                pltpu.VMEM((4, CH, FEAT), BF16),
                pltpu.VMEM((4, CH, COLS), BF16),
                pltpu.VMEM((FEAT, ROWS), BF16),
                pltpu.VMEM((NQ, COLS, CH), BF16),
                pltpu.VMEM((COLS, CH), BF16),
                pltpu.VMEM((CH, 128), F32),
                pltpu.VMEM((1, ROWS), F32),
                pltpu.VMEM((COLS, ROWS), F32),
                pltpu.VMEM((COLS, ROWS), F32),
                pltpu.VMEM((NS, CH, ROWS), BF16),
                dma, dma, dma, dma,
                *[dma((NB + len(PIECES) - 1,))] * 14,
                dma((2,)), dma((2,)), dma((NS,)), dma((NS,)),
            ],
            compiler_params=pltpu.CompilerParams(
                collective_id=0, has_side_effects=True, vmem_limit_bytes=67043328),
            name="two_products",
        )(x_loc.reshape(NB, CH, FEAT), v_loc.reshape(NB, CH, COLS), length_scale, out_scale)
        return out[0].T

    row_spec = P(("task", "row"), None)
    return jax.shard_map(local_program, mesh=mesh, in_specs=(row_spec, row_spec, P("task"), P("task")),
                         out_specs=row_spec, check_vma=False)
```

```python
import jax
import jax.numpy as jnp
from jax import lax
from jax.experimental import pallas as pl
from jax.experimental.pallas import tpu as pltpu
from jax.sharding import PartitionSpec as P

MESH = pl.DeviceIdType.MESH
F32 = jnp.float32
BF16 = jnp.bfloat16
LOG2E = 1.4426950408889634

ROWS = 4096
FEAT = 768
COLS = 128
CH = 512
NB = ROWS // CH
NQ = 4 * NB
NM = NQ - 1
NL = NQ - 2
TI = 256
NT = ROWS // TI
HALF = CH // 2
LATE = 26
PIECES = ((0, 256, 0, 0), (256, 128, 1, 0), (384, 128, 1, 256))
NS = 11
NSTREAM = 3
NH = NQ - (NS - NSTREAM)


def body(x_ref, v_ref, ell_ref, s_ref, w_ref, k_hbm, xg, vg,
         xbuf, vbuf, xt, yg, vt, hj, hi, acc, wacc, slots,
         px_s, px_r, pv_s, pv_r, x_s, x_r, v_s, v_r, fx_s, fx_r, fv_s, fv_r,
         yp_s, yp_r, yx_s, yx_r, yf_s, yf_r, st_sem, sv_sem, ko_sem, kl_sem):
    task = lax.axis_index("task")
    me = lax.axis_index("row")
    partner = me + 1 - 2 * lax.rem(me, 2)
    peer = lax.rem(me + 2, 4)

    barrier = pltpu.get_barrier_semaphore()
    for dev in (peer, partner):
        pl.semaphore_signal(barrier, inc=1, device_id=(task, dev), device_id_type=MESH)
    pl.semaphore_wait(barrier, 2)

    def remote(src, dst, send, recv, dev):
        return pltpu.make_async_remote_copy(
            src_ref=src, dst_ref=dst, send_sem=send, recv_sem=recv,
            device_id=(task, dev), device_id_type=MESH)

    def x_cross(k):
        return remote(x_ref.at[k], xg.at[8 + 2 * k], x_s.at[k], x_r.at[k], peer)

    def v_cross(k):
        return remote(v_ref.at[k], vg.at[8 + 2 * k], v_s.at[k], v_r.at[k], peer)

    def x_fwd(k):
        return remote(xg.at[8 + 2 * k], xg.at[9 + 2 * k], fx_s.at[k], fx_r.at[k], partner)

    def v_fwd(k):
        return remote(vg.at[8 + 2 * k], vg.at[9 + 2 * k], fv_s.at[k], fv_r.at[k], partner)

    last = NB - 1
    x_last, v_last, y_last, x_last_fwd, v_last_fwd, y_last_fwd = [], [], [], [], [], []
    for i, (row, size, c, to) in enumerate(PIECES):
        src, dst, fwd = pl.ds(row, size), pl.ds(to, size), pl.ds(to + size, size)
        n = last + i
        x_last.append(remote(x_ref.at[last, src], xbuf.at[2 + c, dst], x_s.at[n], x_r.at[n], peer))
        v_last.append(remote(v_ref.at[last, src], vbuf.at[2 + c, dst], v_s.at[n], v_r.at[n], peer))
        y_last.append(remote(yg.at[last, :, src], yg.at[NL + c, :, dst], yx_s.at[n], yx_r.at[n], peer))
        x_last_fwd.append(remote(xbuf.at[2 + c, dst], xbuf.at[2 + c, fwd], fx_s.at[n], fx_r.at[n], partner))
        v_last_fwd.append(remote(vbuf.at[2 + c, dst], vbuf.at[2 + c, fwd], fv_s.at[n], fv_r.at[n], partner))
        y_last_fwd.append(remote(yg.at[NL + c, :, dst], yg.at[NL + c, :, fwd], yf_s.at[n], yf_r.at[n], partner))

    def receive_last(i):
        x_last[i].wait_recv()
        x_last_fwd[i].start()
        v_last[i].wait_recv()
        v_last_fwd[i].start()
        x_last_fwd[i].wait_recv()
        v_last_fwd[i].wait_recv()

    x_part = remote(x_ref, xg.at[pl.ds(0, NB)], px_s, px_r, partner)
    v_part = remote(v_ref, vg.at[pl.ds(0, NB)], pv_s, pv_r, partner)

    def y_part(k):
        return remote(yg.at[k], yg.at[NB + k], yp_s.at[k], yp_r.at[k], partner)

    def y_cross(k):
        return remote(yg.at[k], yg.at[16 + 2 * k], yx_s.at[k], yx_r.at[k], peer)

    def y_fwd(k):
        return remote(yg.at[16 + 2 * k], yg.at[17 + 2 * k], yf_s.at[k], yf_r.at[k], partner)

    class Stage:
        def __init__(self, x_src, v_src, buf):
            self.x = pltpu.make_async_copy(x_src, xbuf.at[buf], st_sem.at[buf])
            self.v = pltpu.make_async_copy(v_src, vbuf.at[buf], sv_sem.at[buf])

        def start(self):
            self.x.start()
            self.v.start()

        def wait(self):
            self.x.wait()
            self.v.wait()

    def stage_own(q):
        return Stage(x_ref.at[q], v_ref.at[q], lax.rem(q, 2))

    def stage_got(q):
        return Stage(xg.at[q - NB], vg.at[q - NB], lax.rem(q, 2))

    def k_out(q):
        slot = lax.rem(q, NS)
        return pltpu.make_async_copy(slots.at[slot], k_hbm.at[q], ko_sem.at[slot])

    def stream_slot(q):
        return lax.rem(NH - NSTREAM + lax.rem(q, NSTREAM), NS)

    def k_load(q):
        slot = stream_slot(q)
        return pltpu.make_async_copy(k_hbm.at[q], slots.at[slot], kl_sem.at[slot])

    stage_own(0).start()

    @pl.loop(0, last)
    def _(k):
        v_cross(k).start()
        x_cross(k).start()

    for v, x in zip(v_last, x_last):
        v.start()
        x.start()
    v_part.start()
    x_part.start()

    @pl.loop(0, NB)
    def _(k):
        @pl.when(k + 1 < NB)
        def _():
            stage_own(k + 1).start()

        stage_own(k).wait()
        xct = xbuf[lax.rem(k, 2)].T
        cols = pl.ds(pl.multiple_of(k * CH, CH), CH)
        xt[:, cols] = xct
        hi[:, cols] = 0.5 * jnp.sum(jnp.square(xct.astype(F32)), axis=0, keepdims=True)

    stage_own(0).start()
    acc[...] = jnp.zeros_like(acc)
    wacc[...] = jnp.zeros_like(wacc)

    ell = ell_ref[0]
    s = s_ref[0]
    ratio = jnp.full((8, 128), -2.0 * LOG2E, F32) / jnp.full((8, 128), 2.0 * ell * ell, F32)
    scale_e = ratio[0:1, :]

    def prepare(x_i, rows):
        vt[:, rows] = vbuf[x_i, rows].T
        hj[rows] = jnp.broadcast_to(
            0.5 * jnp.sum(jnp.square(xbuf[x_i, rows].astype(F32)), axis=1, keepdims=True), (rows.size, 128))

    def gen(x_i, rows, slot, cols, width):
        g = jnp.dot(xbuf[x_i, rows], xt[:, cols], preferred_element_type=F32)
        h = jnp.concatenate([hj[rows]] * (width // 128), axis=1)
        c = jnp.concatenate([scale_e] * (width // 128), axis=1)
        d = jnp.maximum(h + hi[:, cols] - g, 0.0)
        slots[slot, rows, cols] = (s * jnp.exp2(d * c)).astype(BF16)

    every = pl.ds(0, CH)

    @pl.loop(0, NM)
    def _(q):
        slot = lax.rem(q, NS)
        n = q + 1
        k = lax.div(n - 16, 2)

        @pl.when(jnp.logical_and(q >= 1, q - 1 < NH))
        def _():
            k_out(q - 1).start()

        @pl.when(q >= NS)
        def _():
            k_out(q - NS).wait()

        @pl.when(q >= NM - NSTREAM)
        def _():
            i = q - (NM - NSTREAM)
            k_out(NH - NSTREAM + i).wait()
            k_load(i).start()

        @pl.when(n < NB)
        def _():
            stage_own(n).start()

        @pl.when(n == NB)
        def _():
            x_part.wait_recv()
            v_part.wait_recv()

        def receive():
            v_cross(k).wait_recv()
            v_fwd(k).start()
            x_cross(k).wait_recv()
            x_fwd(k).start()

        from_peer = jnp.logical_and(n >= 16, lax.rem(n, 2) == 0)
        is_late = jnp.logical_and(jnp.logical_and(from_peer, n >= LATE), n < NL)

        @pl.when(jnp.logical_and(from_peer, n < LATE))
        def _():
            receive()

        @pl.when(jnp.logical_and(jnp.logical_and(n >= 16, lax.rem(n, 2) == 1), n < NL))
        def _():
            v_fwd(k).wait_recv()
            x_fwd(k).wait_recv()

        @pl.when(jnp.logical_and(jnp.logical_and(n >= NB, n < NL), jnp.logical_not(is_late)))
        def _():
            stage_got(n).start()

        @pl.when(q < NL)
        def _():
            stage_own(lax.rem(q, 2)).wait()

        @pl.when(q == NL)
        def _():
            receive_last(0)

        x_i = jnp.where(q < NL, lax.rem(q, 2), 2)
        prepare(x_i, every)

        def app(t):
            cols = pl.ds(t * TI, TI)
            acc[:, cols] += jnp.dot(vt[...], slots[slot, :, cols], preferred_element_type=F32)

        for t in range(NT + 2):
            if t < NT:
                gen(x_i, every, slot, pl.ds(t * TI, TI), TI)
            if t >= 2:
                app(t - 2)

        @pl.when(is_late)
        def _():
            receive()
            stage_got(n).start()

    early, late = pl.ds(0, HALF), pl.ds(HALF, HALF)
    slot_b = (NQ - 1) % NS
    receive_last(1)
    k_out(NQ - 1 - NS).wait()
    prepare(3, early)

    for t in range(NT):
        gen(3, early, slot_b, pl.ds(t * TI, TI), TI)

    receive_last(2)
    prepare(3, late)

    def finish(t):
        cols = pl.ds(pl.multiple_of(t * CH, CH), CH)
        gen(3, late, slot_b, cols, CH)
        y = acc[:, cols] + jnp.dot(vt[...], slots[slot_b, :, cols], preferred_element_type=F32)
        yg[t] = y.astype(BF16)

    def second(q, slot, tiles=range(ROWS // 512), rows=every):
        for t in tiles:
            cols = pl.ds(t * 512, 512)
            wacc[:, cols] += jnp.dot(yg[q, :, rows], slots[slot, rows, cols], preferred_element_type=F32)

    def second_streamed(q):
        k_load(q).wait()
        second(q, stream_slot(q))

        @pl.when(q + NSTREAM < NH)
        def _():
            k_load(q + NSTREAM).start()

    finish(0)

    @pl.loop(1, NB)
    def _(t):
        y_cross(t - 1).start()
        y_part(t - 1).start()
        k_load(t - 1).wait()
        finish(t)
        second(t - 1, stream_slot(t - 1))
        k_load(t - 1 + NSTREAM).start()

    for c in y_last:
        c.start()
    y_part(last).start()
    second_streamed(last)

    def forward_y(k):
        y_cross(k).wait_recv()
        y_fwd(k).start()

    @pl.loop(0, NB)
    def _(i):
        @pl.when(i < 3)
        def _():
            forward_y(i)

        @pl.when(jnp.logical_or(i == 4, i == 6))
        def _():
            forward_y(1 + lax.div(i, 2))

        y_part(i).wait_recv()
        second_streamed(NB + i)

    @pl.loop(0, last)
    def _(i):
        q, r = 16 + i, NH + i
        k = lax.div(i, 2)

        @pl.when(jnp.logical_or(i == 2, i == 3))
        def _():
            forward_y(3 + i)

        for j in range(len(PIECES)):
            @pl.when(i == 4 + j)
            def _():
                y_last[j].wait_recv()
                y_last_fwd[j].start()

        @pl.when(lax.rem(i, 2) == 1)
        def _():
            y_fwd(k).wait_recv()
            y_fwd(k + 4).wait_recv()

        @pl.when(i == 6)
        def _():
            y_last_fwd[0].wait_recv()

        k_load(q).wait()
        sq, sr = stream_slot(q), lax.rem(r, NS)
        for t in range(ROWS // 512):
            cols = pl.ds(t * 512, 512)
            wacc[:, cols] += (jnp.dot(yg[q], slots[sq, :, cols], preferred_element_type=F32)
                              + jnp.dot(yg[r], slots[sr, :, cols], preferred_element_type=F32))

        @pl.when(q + NSTREAM < NH)
        def _():
            k_load(q + NSTREAM).start()

    y_fwd(3).wait_recv()
    y_last_fwd[1].wait_recv()
    second(NQ - 1, slot_b, rows=early)
    y_last_fwd[2].wait_recv()
    second(NQ - 1, slot_b, rows=late)
    k_load(NH - 1).wait()

    n_out = 8
    width = ROWS // n_out
    outs = [pltpu.make_async_copy(wacc.at[:, pl.ds(b * width, width)], w_ref.at[:, pl.ds(b * width, width)],
                                  kl_sem.at[b]) for b in range(n_out)]
    for b in range(n_out):
        second(NH - 1, (NH - 1) % NS, (b,))
        if b:
            outs[b - 1].start()

    x_part.wait_send()
    v_part.wait_send()
    outs[-1].start()

    @pl.loop(0, last)
    def _(k):
        x_cross(k).wait_send()
        v_cross(k).wait_send()
        x_fwd(k).wait_send()
        v_fwd(k).wait_send()

    for c in (*x_last, *x_last_fwd, *v_last, *v_last_fwd, *y_last, *y_last_fwd):
        c.wait_send()

    @pl.loop(0, last)
    def _(k):
        y_part(k).wait_send()
        y_cross(k).wait_send()
        y_fwd(k).wait_send()

    y_part(last).wait_send()

    for o in outs:
        o.wait()


def solution(mesh):
    def local_program(x_loc, v_loc, length_scale, out_scale):
        dma = pltpu.SemaphoreType.DMA
        any_spec = pl.BlockSpec(memory_space=pl.ANY)
        smem = pl.BlockSpec(memory_space=pltpu.SMEM)
        out = pl.pallas_call(
            body,
            out_shape=[
                jax.ShapeDtypeStruct((COLS, ROWS), F32),
                jax.ShapeDtypeStruct((NH, CH, ROWS), BF16),
                jax.ShapeDtypeStruct((NL - NB, CH, FEAT), BF16),
                jax.ShapeDtypeStruct((NL - NB, CH, COLS), BF16),
            ],
            in_specs=[any_spec, any_spec, smem, smem],
            out_specs=[any_spec] * 4,
            scratch_shapes=[
                pltpu.VMEM((4, CH, FEAT), BF16),
                pltpu.VMEM((4, CH, COLS), BF16),
                pltpu.VMEM((FEAT, ROWS), BF16),
                pltpu.VMEM((NQ, COLS, CH), BF16),
                pltpu.VMEM((COLS, CH), BF16),
                pltpu.VMEM((CH, 128), F32),
                pltpu.VMEM((1, ROWS), F32),
                pltpu.VMEM((COLS, ROWS), F32),
                pltpu.VMEM((COLS, ROWS), F32),
                pltpu.VMEM((NS, CH, ROWS), BF16),
                dma, dma, dma, dma,
                *[dma((NB + len(PIECES) - 1,))] * 14,
                dma((2,)), dma((2,)), dma((NS,)), dma((NS,)),
            ],
            compiler_params=pltpu.CompilerParams(
                collective_id=0, has_side_effects=True, vmem_limit_bytes=67043328),
            name="two_products",
        )(x_loc.reshape(NB, CH, FEAT), v_loc.reshape(NB, CH, COLS), length_scale, out_scale)
        return out[0].T

    row_spec = P(("task", "row"), None)
    return jax.shard_map(local_program, mesh=mesh, in_specs=(row_spec, row_spec, P("task"), P("task")),
                         out_specs=row_spec, check_vma=False)
```
